256 devices in a mesh: depth: 8 (over y, core), lat: 32 (over z, x).
Axes of the slice: x: 4, y: 4, z: 8, core: 2. Of those that a mesh axis runs over, the one named last changes fastest.
Arguments:
- fields: float32 [8, 2, 2, 2, 512, 512], P('depth', None, None, None, 'lat'), may hold values from -6 to 6
- surface: float32 [2, 2, 2, 512, 512], P(None, None, None, 'lat'), may hold values from -6 to 6
- held_freqs: int32 [8, 2], P('depth'), may hold values from 8 to 63
- surface_freqs: int32 [2], replicated, may hold values from 8 to 63
- ref_slowness: float32 [8, 1, 2], P('depth'), may hold values from 0.6 to 1.2
- weights: float32 [8, 1, 512, 512], P('depth', None, 'lat'), may hold values from 0 to 1
- regions: int32 [8, 1, 512, 512], P('depth', None, 'lat'), may hold values from 0 to 7
- region_slowness: float32 [8, 1, 8], P('depth'), may hold values from 0.6 to 1.2
Outputs:
- fields_out: float32 [8, 2, 2, 2, 512, 512], P('depth', None, None, None, 'lat')
- image_out: float32 [8, 1, 16, 512, 512], P('depth', None, None, 'lat')
The draws below stay inside these ranges and needn't reach their ends.
All inputs are finite; a program needn't handle non-finite values.
Results may differ from the reference program's by a relative error of at most 0.0003.
Values sent between devices are 32-bit elements; how exact they have to be, the bound alone decides.
No kernel may reach another device: no remote copies, remote signals or barrier semaphores. Data moves between devices by JAX's collectives and lax.ppermute only.
A program may use at most 64 MiB of HBM per device.

```python
import math
import jax
import jax.numpy as jnp
from jax import lax

NX = 512
NY = 512
FREQ = 2
LEVELS = 1
LAGS = 16
REGIONS = 8
SECTIONS = 8


def plant(drawn, stream_key, low, top_value):
    index_at = [jax.random.randint(jax.random.fold_in(stream_key, axis), (), 0, length) for axis, length in enumerate(drawn.shape)]
    main_axis = drawn.shape.index(max(drawn.shape))
    next_to = index_at[:main_axis] + [(index_at[main_axis] + 1) % drawn.shape[main_axis]] + index_at[main_axis + 1:]
    return drawn.at[tuple(index_at)].set(low).at[tuple(next_to)].set(top_value)


def shard_levels(key, dims, pieces, least, top_value):
    loudness, own = 1.0, jax.random.fold_in(key, 6)
    for axis_at, shards_of in pieces:
        heights = jnp.exp(jax.random.uniform(jax.random.fold_in(own, axis_at), (shards_of,), jnp.float32, least / len(pieces), top_value / len(pieces)))
        loudness = loudness * jnp.repeat(heights, dims[axis_at] // shards_of).reshape([-1 if axis == axis_at else 1 for axis in range(len(dims))])
    return loudness


def centred(stream_key, dims, width, reach, cuts=(), kind=jnp.bfloat16):
    result = width * jax.random.normal(stream_key, dims, jnp.float32)
    if cuts:
        result = result * shard_levels(stream_key, dims, cuts, -0.22, 0.18)
    return jnp.clip(result, -reach, reach).astype(kind)


def setup_inputs(seed: int = 0) -> dict:
    keys = jax.random.split(jax.random.key(seed), 9)
    return {
        "fields": centred(keys[0], (SECTIONS, 2, 2, FREQ, NX, NY), 1.0, 6.0, ((0, 8), (4, 32)), jnp.float32),
        "surface": centred(keys[1], (2, 2, FREQ, NX, NY), 1.0, 6.0, ((3, 32),), jnp.float32),
        "held_freqs": plant(jax.random.randint(keys[2], (SECTIONS, FREQ), 8, 64), jax.random.fold_in(keys[2], 1), 8, 63).astype(jnp.int32),
        "surface_freqs": jax.random.randint(keys[3], (FREQ,), 8, 64).astype(jnp.int32),
        "ref_slowness": jnp.clip(0.6 + 0.6 * jax.random.uniform(keys[4], (SECTIONS, LEVELS, 2), jnp.float32) ** shard_levels(keys[4], (SECTIONS, LEVELS, 2), ((0, 8),), -0.2, 0.2), 0.6, 1.2),
        "weights": jnp.clip(1.0 * jax.random.uniform(keys[5], (SECTIONS, LEVELS, NX, NY), jnp.float32) ** shard_levels(keys[5], (SECTIONS, LEVELS, NX, NY), ((0, 8), (2, 32)), -0.2, 0.2), 0.0, 1.0),
        "regions": plant(jax.random.randint(keys[6], (SECTIONS, LEVELS, NX, NY), 0, REGIONS), jax.random.fold_in(keys[6], 1), 0, REGIONS - 1).astype(jnp.int32),
        "region_slowness": jnp.clip(0.6 + 0.6 * jax.random.uniform(keys[7], (SECTIONS, LEVELS, REGIONS), jnp.float32) ** shard_levels(keys[7], (SECTIONS, LEVELS, REGIONS), ((0, 8),), -0.2, 0.2), 0.6, 1.2),
    }


omega_step = 0.04
depth_step = 1.0

def wave_numbers(length):
    positions = jnp.arange(length, dtype=jnp.int32)
    folded = jnp.where(positions < length // 2, positions, positions - length)
    return folded.astype(jnp.float32) * (2.0 * math.pi / length)

def level_step(wave_field, omega_batch, slow_pair, weight, cell_slow, sign_pair):
    wave_x = wave_numbers(NX)
    wave_y = wave_numbers(NY)
    squared = wave_x[:, None] ** 2 + wave_y[None, :] ** 2
    spectrum = jnp.fft.fft2(wave_field, axes=(-2, -1))
    ref_fields = []
    for ref_index in range(2):
        wave_base = omega_batch[:, None, None] * slow_pair[ref_index]
        wave_gap = wave_base * wave_base - squared[None]
        amplitude = jnp.exp(-jnp.sqrt(jnp.maximum(-wave_gap, 0.0)) * depth_step)
        turning = sign_pair[:, None, None, None] * jnp.sqrt(jnp.maximum(wave_gap, 0.0))[None] * depth_step
        factor = lax.complex(amplitude[None] * jnp.cos(turning), amplitude[None] * jnp.sin(turning))
        ref_fields.append(jnp.fft.ifft2(spectrum * factor, axes=(-2, -1)))
    mixed_field = weight * ref_fields[0] + (1.0 - weight) * ref_fields[1]
    blend_slow = weight * slow_pair[0] + (1.0 - weight) * slow_pair[1]
    lens_angle = sign_pair[:, None, None, None] * omega_batch[None, :, None, None] * (cell_slow - blend_slow)[None, None] * depth_step
    return mixed_field * lax.complex(jnp.cos(lens_angle), jnp.sin(lens_angle))

def image_terms(wave_field):
    half_lags = LAGS // 2
    row_count = wave_field.shape[-2]
    source = jnp.pad(wave_field[0], ((0, 0), (half_lags, half_lags), (0, 0)))
    receiver = jnp.pad(wave_field[1], ((0, 0), (half_lags, half_lags), (0, 0)))
    lag_terms = []
    for lag_index in range(LAGS):
        offset = lag_index - half_lags
        source_rows = source[:, half_lags - offset:half_lags - offset + row_count]
        receiver_rows = receiver[:, half_lags + offset:half_lags + offset + row_count]
        product = jnp.real(source_rows) * jnp.real(receiver_rows) + jnp.imag(source_rows) * jnp.imag(receiver_rows)
        lag_terms.append(lax.optimization_barrier(jnp.sum(product, axis=0)))
    return jnp.stack(lag_terms)

def reference(fields, surface, held_freqs, surface_freqs, ref_slowness, weights, regions, region_slowness):
    sign_pair = jnp.array([-1.0, 1.0], dtype=jnp.float32)
    sections = fields.shape[0]
    held_waves = [lax.complex(fields[section, 0], fields[section, 1]) for section in range(sections)]
    omegas = [held_freqs[section].astype(jnp.float32) * omega_step for section in range(sections)]
    cells = [[jnp.take(region_slowness[section, level_index], regions[section, level_index]) for level_index in range(LEVELS)] for section in range(sections)]
    images = [[None for level_index in range(LEVELS)] for section in range(sections)]
    results = []
    for tick_index in range(2):
        results = []
        for section in range(sections):
            wave_field = held_waves[section]
            for level_index in range(LEVELS):
                wave_field = level_step(wave_field, omegas[section], ref_slowness[section, level_index], weights[section, level_index], cells[section][level_index], sign_pair)
                lag_term = image_terms(wave_field)
                if tick_index == 0:
                    images[section][level_index] = lag_term
                else:
                    images[section][level_index] = images[section][level_index] + lag_term
            results.append(wave_field)
        if tick_index == 0:
            held_waves = [lax.complex(surface[0], surface[1])] + results[:-1]
            omegas = [surface_freqs.astype(jnp.float32) * omega_step] + omegas[:-1]
    fields_out = jnp.stack([jnp.stack([jnp.real(wave_field), jnp.imag(wave_field)]) for wave_field in results])
    image_out = jnp.stack([jnp.stack(images[section]) for section in range(sections)])
    return (fields_out, image_out)
```

```python
import functools
import math

import jax
import jax.numpy as jnp
import ml_dtypes
import numpy as np
from jax import lax
from jax.experimental import pallas as pl
from jax.experimental.pallas import tpu as pltpu
from jax.sharding import PartitionSpec as P

LAGS = 16
HALF = LAGS // 2
REGIONS = 8
CHUNK = 16
LANES = 128
INTERPRET = False

omega_step = 0.04
depth_step = 1.0

COS_TERMS = [(-1.0) ** n / math.factorial(2 * n) for n in range(13)]
SIN_TERMS = [(-1.0) ** n / math.factorial(2 * n + 1) for n in range(13)]


def polynomial(value, terms):
    total = jnp.full_like(value, terms[-1])
    for term in terms[-2::-1]:
        total = total * value + term
    return total


def transform_table(length):
    index = np.arange(length)
    angle = 2.0 * np.pi * (index[:, None] * index[None, :] % length) / length
    table = np.concatenate([np.cos(angle), np.sin(angle)], axis=1)
    lead = table.astype(ml_dtypes.bfloat16)
    trail = (table - lead.astype(np.float64)).astype(ml_dtypes.bfloat16)
    return lead, trail


def two_parts(value):
    lead = value.astype(jnp.bfloat16)
    return lead, (value - lead.astype(jnp.float32)).astype(jnp.bfloat16)


def dot(left, right):
    return jnp.dot(left, right, preferred_element_type=jnp.float32)


def dot_rows(value, lead_ref, trail_ref):
    lead, trail = two_parts(value)
    return dot(lead, lead_ref[...]) + (dot(trail, lead_ref[...]) + dot(lead, trail_ref[...]))


def dot_columns(lead_ref, trail_ref, value, length):
    lead, trail = two_parts(value)
    results = []
    for part in range(2):
        at = pl.ds(part * length, length)
        results.append(
            dot(lead_ref[:, at], lead) + (dot(lead_ref[:, at], trail) + dot(trail_ref[:, at], lead))
        )
    return results


def swap_chunks(pieces):
    pieces = list(pieces)
    lane = lax.broadcasted_iota(jnp.int32, pieces[0].shape, 1)
    for bit in (1, 2, 4):
        upper = (lane // (CHUNK * bit)) % 2 == 1
        for low in range(8):
            if low & bit:
                continue
            first, second = pieces[low], pieces[low | bit]
            pieces[low] = jnp.where(upper, pltpu.roll(second, CHUNK * bit, 1), first)
            pieces[low | bit] = jnp.where(upper, second, pltpu.roll(first, LANES - CHUNK * bit, 1))
    return pieces


def rows_to_blocks(value, lead_ref, trail_ref, out_ref, rows):
    length = value.shape[1]
    half = value.shape[0] // 2
    both = dot_rows(value, lead_ref, trail_ref)
    cos_part, sin_part = both[:, :length], both[:, length:]
    spectrum = (cos_part[:half] + sin_part[half:], cos_part[half:] - sin_part[:half])
    for tile in range(length // LANES):
        lanes = slice(tile * LANES, (tile + 1) * LANES)
        pieces = [
            spectrum[part][group * rows : (group + 1) * rows, lanes]
            for part in range(2)
            for group in range(half // rows)
        ]
        for block, piece in enumerate(swap_chunks(pieces)):
            out_ref[pl.ds((tile * 8 + block) * rows, rows), :] = piece


def rows_kernel(field_ref, lead_ref, trail_ref, out_ref, *, rows):
    rows_to_blocks(field_ref[...], lead_ref, trail_ref, out_ref, rows)


def factor_kernel(freq_ref, slow_ref, block_ref, even_ref, odd_ref, *, length, col_length):
    shape = (length, LANES)
    row = lax.broadcasted_iota(jnp.int32, shape, 0)
    lane = lax.broadcasted_iota(jnp.int32, shape, 1)
    step_x, step_y = 2.0 * math.pi / length, 2.0 * math.pi / col_length
    wave_x = jnp.where(row < length // 2, row, row - length).astype(jnp.float32) * step_x
    col = block_ref[0] * CHUNK + lane % CHUNK
    wave_y = jnp.where(col < col_length // 2, col, col - col_length).astype(jnp.float32) * step_y
    squared = wave_x * wave_x + wave_y * wave_y
    omega = jnp.where((lane // CHUNK) % 2 == 0, freq_ref[0], freq_ref[1])
    is_source = (lane // (2 * CHUNK)) % 2 == 0
    is_real = lane < LANES // 2
    direction = jnp.where(is_source == is_real, 1.0, -1.0)
    for ref in range(2):
        base = omega * slow_ref[ref]
        gap = base * base - squared
        fade = jnp.exp(-jnp.sqrt(jnp.maximum(-gap, 0.0)) * depth_step)
        inside = jnp.maximum(gap, 0.0)
        even_ref[ref] = fade * polynomial(inside, COS_TERMS)
        odd_ref[ref] = direction * (fade * (jnp.sqrt(inside) * polynomial(inside, SIN_TERMS)))


def columns_kernel(in_ref, even_ref, odd_ref, lead_ref, trail_ref, out_ref):
    length = in_ref.shape[0]
    lane = lax.broadcasted_iota(jnp.int32, (length, LANES), 1)
    turn = jnp.where(lane < LANES // 2, 1.0, -1.0)
    cos_part, sin_part = dot_columns(lead_ref, trail_ref, in_ref[...], length)
    spectrum = cos_part + turn * pltpu.roll(sin_part, LANES // 2, 1)
    swapped = pltpu.roll(spectrum, LANES // 2, 1)
    shifted = [spectrum * even_ref[ref] + swapped * odd_ref[ref] for ref in range(2)]
    cos_part, sin_part = dot_columns(
        lead_ref, trail_ref, jnp.concatenate(shifted, axis=1), length
    )
    for ref in range(2):
        lanes = slice(ref * LANES, (ref + 1) * LANES)
        out_ref[:, lanes] = cos_part[:, lanes] - turn * pltpu.roll(
            sin_part[:, lanes], LANES // 2, 1
        )


def continued(in_ref, lens_ref, weight_ref, lead_ref, trail_ref, rows):
    length = lead_ref.shape[0]
    tiles = []
    for tile in range(length // LANES):
        column = []
        for ref in range(2):
            column += swap_chunks(
                [
                    in_ref[pl.ds((tile * 8 + block) * rows, rows), ref * LANES : (ref + 1) * LANES]
                    for block in range(8)
                ]
            )
        tiles.append(jnp.concatenate(column, axis=0))
    both = dot_rows(jnp.concatenate(tiles, axis=1), lead_ref, trail_ref)
    cos_part, sin_part = both[:, :length], both[:, length:]
    half = 4 * rows
    weight = weight_ref[...]
    real, imag = [], []
    for group in range(4):
        parts = []
        for ref in range(2):
            at_real = ref * 2 * half + group * rows
            at_imag = at_real + half
            parts.append(
                (
                    cos_part[at_real : at_real + rows] - sin_part[at_imag : at_imag + rows],
                    cos_part[at_imag : at_imag + rows] + sin_part[at_real : at_real + rows],
                )
            )
        mixed = [weight * parts[0][p] + (1.0 - weight) * parts[1][p] for p in range(2)]
        lens_cos = lens_ref[0, group % 2]
        lens_sin = lens_ref[1, group % 2] if group >= 2 else -lens_ref[1, group % 2]
        real.append(mixed[0] * lens_cos - mixed[1] * lens_sin)
        imag.append(mixed[0] * lens_sin + mixed[1] * lens_cos)
    return jnp.concatenate(real + imag, axis=0)


def turn_kernel(
    in_ref, lens_ref, weight_ref, surface_ref, last_ref, lead_ref, trail_ref, field_ref, out_ref, *, rows
):
    field = continued(in_ref, lens_ref, weight_ref, lead_ref, trail_ref, rows)
    field_ref[...] = field
    start = jnp.where(last_ref[0] == 1, surface_ref[...], field)
    rows_to_blocks(start, lead_ref, trail_ref, out_ref, rows)


def end_kernel(in_ref, lens_ref, weight_ref, lead_ref, trail_ref, field_ref, *, rows):
    field_ref[...] = continued(in_ref, lens_ref, weight_ref, lead_ref, trail_ref, rows)


def image_body(field_ref, above_ref, below_ref, base_ref, out_ref, padded_ref, rows):
    for index in range(8):
        padded_ref[index, pl.ds(0, HALF)] = above_ref[index]
        padded_ref[index, pl.ds(HALF, rows)] = field_ref[index]
        padded_ref[index, pl.ds(HALF + rows, HALF)] = below_ref[index]
    for lag in range(LAGS):
        offset = lag - HALF
        total = None if base_ref is None else base_ref[lag]
        for part in range(2):
            for freq in range(2):
                source = padded_ref[part * 4 + freq, pl.ds(HALF - offset, rows)]
                receiver = padded_ref[part * 4 + 2 + freq, pl.ds(HALF + offset, rows)]
                total = source * receiver if total is None else total + source * receiver
        out_ref[lag] = total


def image_first(field_ref, above_ref, below_ref, out_ref, padded_ref, *, rows):
    image_body(field_ref, above_ref, below_ref, None, out_ref, padded_ref, rows)


def image_second(field_ref, above_ref, below_ref, base_ref, out_ref, padded_ref, *, rows):
    image_body(field_ref, above_ref, below_ref, base_ref, out_ref, padded_ref, rows)


VMEM = pl.BlockSpec(memory_space=pltpu.VMEM)
SMEM = pl.BlockSpec(memory_space=pltpu.SMEM)


def call(kernel, name, in_specs, out_shapes, operands, flops, scratch=(), **params):
    many = len(out_shapes) > 1
    shapes = [jax.ShapeDtypeStruct(shape, jnp.float32) for shape in out_shapes]
    return pl.pallas_call(
        functools.partial(kernel, **params),
        name=name,
        in_specs=in_specs,
        out_specs=[VMEM] * len(shapes) if many else VMEM,
        out_shape=shapes if many else shapes[0],
        scratch_shapes=list(scratch),
        cost_estimate=pl.CostEstimate(flops=flops, bytes_accessed=1 << 20, transcendentals=0),
        compiler_params=pltpu.CompilerParams(vmem_limit_bytes=24 << 20),
        interpret=INTERPRET,
    )(*operands)


def exchanged(value):
    return lax.all_to_all(value, "lat", split_axis=0, concat_axis=0, tiled=True)


def shards(
    fields, surface, held_freqs, surface_freqs, ref_slowness, weights, regions, region_slowness
):
    lane_count = lax.axis_size("lat")
    sections = lax.axis_size("depth")
    rows, col_length = fields.shape[4], fields.shape[5]
    length = lane_count * rows
    table_y = [jnp.asarray(part) for part in transform_table(col_length)]
    table_x = table_y if length == col_length else [jnp.asarray(p) for p in transform_table(length)]
    flat = (8 * rows, col_length)
    block = lax.axis_index("lat").reshape(1)
    at_end = lax.axis_index("depth") == sections - 1

    region_ids = jnp.arange(REGIONS, dtype=jnp.int32)
    matches = (regions[0, 0][None] == region_ids[:, None, None]).astype(jnp.float32)
    cell_slowness = jnp.sum(matches * region_slowness[0, 0][:, None, None], axis=0)
    weight = weights[0, 0]
    slow = ref_slowness[0, 0]
    blend = weight * slow[0] + (1.0 - weight) * slow[1]
    lens_gap = cell_slowness - blend
    upward = [(s, (s - 1) % sections) for s in range(sections)]
    slow_rows = jnp.broadcast_to(slow[:, None, None], (2, 4, col_length)).reshape(8, col_length)
    passed = lax.ppermute(jnp.concatenate([lens_gap, weight, slow_rows], axis=0), "depth", upward)
    next_gap, next_weight = passed[:rows], passed[rows : 2 * rows]
    next_slow = passed[2 * rows :: 4, 0]

    omega = held_freqs[0].astype(jnp.float32) * omega_step
    next_omega = jnp.where(at_end, surface_freqs.astype(jnp.float32) * omega_step, omega)
    scale = 1.0 / (length * col_length)

    def lens_of(freqs, gap):
        angle = freqs[:, None, None] * gap[None] * depth_step
        return jnp.stack([jnp.cos(angle) * scale, jnp.sin(angle) * scale])

    def factors(freqs, slow_pair):
        shape = (2, length, LANES)
        return call(
            factor_kernel,
            "factors",
            [SMEM, SMEM, SMEM],
            [shape, shape],
            (freqs, slow_pair, block),
            1 << 27,
            length=length,
            col_length=col_length,
        )

    def columns(value, pair):
        return call(
            columns_kernel,
            "columns",
            [VMEM] * 5,
            [(length, 2 * LANES)],
            (value, *pair, *table_x),
            1 << 30,
        )

    def edges(field, pairs_of, axes):
        parts = field.reshape(8, rows, col_length)
        down = lax.ppermute(parts[:, rows - HALF :], axes, pairs_of(1))
        up = lax.ppermute(parts[:, :HALF], axes, pairs_of(-1))
        return parts, down, up

    padded = [pltpu.VMEM((8, rows + 2 * HALF, col_length), jnp.float32)]
    image_shape = (LAGS, rows, col_length)

    spectra = call(
        rows_kernel,
        "rows",
        [VMEM] * 3,
        [(length, LANES)],
        (fields[0].reshape(flat), *table_y),
        1 << 29,
        rows=rows,
    )
    spectra = exchanged(spectra)
    returned = exchanged(columns(spectra, factors(omega, slow)))
    field, spectra = call(
        turn_kernel,
        "turn",
        [VMEM] * 4 + [SMEM] + [VMEM] * 2,
        [flat, (length, LANES)],
        (
            returned,
            lens_of(omega, lens_gap),
            weight,
            surface.reshape(flat),
            at_end.astype(jnp.int32).reshape(1),
            *table_y,
        ),
        1 << 30,
        rows=rows,
    )

    def along(step):
        return [(i, i + step) for i in range(lane_count) if 0 <= i + step < lane_count]

    spectra = exchanged(spectra)
    parts, above, below = edges(field, along, "lat")
    image = call(
        image_first, "image", [VMEM] * 3, [image_shape], (parts, above, below), 1 << 26, padded, rows=rows
    )
    returned = exchanged(columns(spectra, factors(next_omega, next_slow)))
    field = call(
        end_kernel,
        "end",
        [VMEM] * 5,
        [flat],
        (returned, lens_of(next_omega, next_gap), next_weight, *table_y),
        1 << 30,
        rows=rows,
    )

    def diagonal(step):
        return [
            (s * lane_count + i, (s + 1) % sections * lane_count + i + step)
            for s in range(sections)
            for i in range(lane_count)
            if 0 <= i + step < lane_count
        ]

    parts, above, below = edges(field, diagonal, ("depth", "lat"))
    parts = lax.ppermute(parts, ("depth", "lat"), diagonal(0))
    image = call(
        image_second,
        "image_sum",
        [VMEM] * 4,
        [image_shape],
        (parts, above, below, image),
        1 << 26,
        padded,
        rows=rows,
    )
    return (parts.reshape(fields.shape), image[None, None])


def solution(mesh):
    in_specs = (
        P("depth", None, None, None, "lat", None),
        P(None, None, None, "lat", None),
        P("depth", None),
        P(),
        P("depth", None, None),
        P("depth", None, "lat", None),
        P("depth", None, "lat", None),
        P("depth", None, None),
    )
    out_specs = (P("depth", None, None, None, "lat", None), P("depth", None, None, "lat", None))
    return jax.shard_map(shards, mesh=mesh, in_specs=in_specs, out_specs=out_specs, check_vma=False)
```

```python
import functools
import math

import jax
import jax.numpy as jnp
import ml_dtypes
import numpy as np
from jax import lax
from jax.experimental import pallas as pl
from jax.experimental.pallas import tpu as pltpu
from jax.sharding import PartitionSpec as P

LAGS = 16
HALF = LAGS // 2
REGIONS = 8
GROUPS = 4
CHUNK = 64
LANES = 128
INTERPRET = False

omega_step = 0.04
depth_step = 1.0

COS_TERMS = [(-1.0) ** n / math.factorial(2 * n) for n in range(12)]
SIN_TERMS = [(-1.0) ** n / math.factorial(2 * n + 1) for n in range(12)]


def polynomial(value, terms):
    total = jnp.full_like(value, terms[-1])
    for term in terms[-2::-1]:
        total = total * value + term
    return total


def transform_tables(length):
    half = length // 2
    index = np.arange(half)
    even = 2.0 * np.pi * (2 * index[:, None] * index[None, :] % length) / length
    odd = 2.0 * np.pi * (index[:, None] * (2 * index[None, :] + 1) % length) / length
    tables = []
    for angles in ([even, odd], [odd.T]):
        table = np.concatenate([f(a) for a in angles for f in (np.cos, np.sin)], axis=1)
        lead = table.astype(ml_dtypes.bfloat16)
        trail = (table - lead.astype(np.float64)).astype(ml_dtypes.bfloat16)
        tables.append(jnp.asarray(np.concatenate([lead, trail], axis=1)))
    return tables


class Table:
    def __init__(self, main_ref, odd_ref=None):
        self.main, self.odd = main_ref, odd_ref
        self.width = main_ref.shape[0]

    def part(self, part, first, count, trail):
        if part == 1 and self.odd is not None:
            start = (2 * trail + first) * self.width
            return self.odd[:, start : start + count * self.width]
        start = (4 * trail + 2 * part + first) * self.width
        return self.main[:, start : start + count * self.width]


def two_parts(value):
    lead = value.astype(jnp.bfloat16)
    return lead, (value - lead.astype(jnp.float32)).astype(jnp.bfloat16)


def dot(left, right):
    return jnp.dot(left, right, preferred_element_type=jnp.float32)


def dot_right(value, table, part):
    width = value.shape[1]
    lead, trail = two_parts(value)
    main, rest = table.part(part, 0, 2, 0), table.part(part, 0, 2, 1)
    both = dot(lead, main) + (dot(trail, main) + dot(lead, rest))
    return both[:, :width], both[:, width:]


def dot_left(table, part, value):
    lead, trail = two_parts(value)
    results = []
    for which in range(2):
        main, rest = table.part(part, which, 1, 0), table.part(part, which, 1, 1)
        results.append(dot(main, lead) + (dot(main, trail) + dot(rest, lead)))
    return results


def joined(pairs, axis):
    return [jnp.concatenate([pair[i] for pair in pairs], axis=axis) for i in range(2)]


def analysed_right(value, table):
    half = value.shape[1] // 2
    low, high = value[:, :half], value[:, half:]
    return joined([dot_right(low + high, table, 0), dot_right(low - high, table, 1)], 1)


def restored_right(value, table):
    half = value.shape[1] // 2
    even, odd = dot_right(value[:, :half], table, 0), dot_right(value[:, half:], table, 1)
    return joined([[e + o for e, o in zip(even, odd)], [e - o for e, o in zip(even, odd)]], 1)


def analysed_left(table, value):
    half = value.shape[0] // 2
    low, high = value[:half], value[half:]
    return joined([dot_left(table, 0, low + high), dot_left(table, 1, low - high)], 0)


def restored_left(table, value):
    half = value.shape[0] // 2
    even, odd = dot_left(table, 0, value[:half]), dot_left(table, 1, value[half:])
    return joined([[e + o for e, o in zip(even, odd)], [e - o for e, o in zip(even, odd)]], 0)


def swap_halves(first, second):
    lane = lax.broadcasted_iota(jnp.int32, first.shape, 1)
    low = lane < CHUNK
    return (
        jnp.where(low, first, pltpu.roll(second, CHUNK, 1)),
        jnp.where(low, pltpu.roll(first, CHUNK, 1), second),
    )


def wave_index(position, length):
    half = length // 2
    index = jnp.where(position < half, 2 * position, 2 * (position - half) + 1)
    return jnp.where(index < half, index, index - length).astype(jnp.float32)


def block_row(index, rows):
    return pl.multiple_of(index * rows, rows)


def my_group():
    lat = lax.axis_index("lat")
    members = lax.axis_size("lat") // GROUPS
    return lax.div(lat, members), lax.rem(lat, members)


def omega_pair(held_ref, surface_ref, tick):
    pair = []
    for freq in range(2):
        number = held_ref[freq]
        if tick == 1:
            at_end = lax.axis_index("depth") == lax.axis_size("depth") - 1
            number = jnp.where(at_end, surface_ref[freq], number)
        pair.append(number.astype(jnp.float32) * omega_step)
    return pair


def my_omega(held_ref, surface_ref, tick):
    pair = omega_pair(held_ref, surface_ref, tick)
    return jnp.where(lax.rem(my_group()[0], 2) == 0, pair[0], pair[1])


def lens(angle, scale):
    square = angle * angle
    return (
        polynomial(square, COS_TERMS) * scale,
        angle * polynomial(square, SIN_TERMS) * scale,
    )


def prepare_kernel(
    regions_ref, region_slow_ref, weights_ref, slow_ref, packed_ref, params_ref, *, rows
):
    regions, weight = regions_ref[...], weights_ref[...]
    cell = jnp.full(weight.shape, region_slow_ref[0])
    for region in range(1, REGIONS):
        cell = jnp.where(regions == region, region_slow_ref[region], cell)
    gap = cell - (weight * slow_ref[0] + (1.0 - weight) * slow_ref[1])
    for out in (packed_ref, params_ref):
        out[pl.ds(0, rows), :] = gap
        out[pl.ds(rows, rows), :] = weight
    for ref in range(2):
        params_ref[pl.ds(2 * rows + 8 * ref, 8), :] = jnp.full((8, weight.shape[1]), slow_ref[ref])


def gather_kernel(held_ref, *refs, rows):
    pieces, (weight_ref, lens_ref) = refs[:GROUPS], refs[GROUPS:]
    group = my_group()[0]
    omega = my_omega(held_ref, None, 0)
    sign = jnp.where(group < 2, -1.0, 1.0)
    scale = 1.0 / (weight_ref.shape[1] * (lax.axis_size("lat") * rows))
    for shift in range(GROUPS):
        piece = pieces[shift]
        source = lax.rem(group - shift + GROUPS, GROUPS)
        at = block_row(source, rows)
        weight_ref[pl.ds(at, rows), :] = piece[pl.ds(rows, rows), :]
        cos_part, sin_part = lens(piece[pl.ds(0, rows), :] * omega * depth_step, scale)
        lens_ref[0, pl.ds(at, rows), :] = cos_part
        lens_ref[1, pl.ds(at, rows), :] = sin_part * sign


def lens_kernel(held_ref, surface_freq_ref, passed_ref, lens_ref, *, rows):
    scale = 1.0 / (passed_ref.shape[1] * (lax.axis_size("lat") * rows))
    for freq, omega in enumerate(omega_pair(held_ref, surface_freq_ref, 1)):
        cos_part, sin_part = lens(passed_ref[pl.ds(0, rows), :] * omega * depth_step, scale)
        lens_ref[0, freq] = cos_part
        lens_ref[1, freq] = sin_part


def rows_kernel(field_ref, surface_ref, table_ref, out_ref, *, rows):
    half = field_ref.shape[0] // 2
    members = field_ref.shape[1] // CHUNK
    value = jnp.concatenate([field_ref[...], surface_ref[...]], axis=0)
    cos_part, sin_part = analysed_right(value, Table(table_ref))
    for batch in range(2):
        at_real = 2 * half * batch
        at_imag = at_real + half
        real = cos_part[at_real:at_imag] + sin_part[at_imag : at_imag + half]
        imag = cos_part[at_imag : at_imag + half] - sin_part[at_real:at_imag]
        out_lanes = slice(batch * LANES, (batch + 1) * LANES)
        for tile in range(field_ref.shape[1] // LANES):
            lanes = slice(tile * LANES, (tile + 1) * LANES)
            for at, block in enumerate(swap_halves(real[:, lanes], imag[:, lanes])):
                for group in range(GROUPS):
                    start = (group * members + 2 * tile + at) * rows
                    out_ref[pl.ds(start, rows), out_lanes] = block[group * rows : (group + 1) * rows]


def factor_kernel(held_ref, surface_ref, params_ref, even_ref, odd_ref, *, tick, length, rows):
    col_length = params_ref.shape[1]
    shape = (length, LANES)
    lane = lax.broadcasted_iota(jnp.int32, (1, LANES), 1)
    group, member = my_group()
    wave_y = wave_index(member * CHUNK + lax.rem(lane, CHUNK), col_length) * (
        2.0 * math.pi / col_length
    )
    row = lax.broadcasted_iota(jnp.int32, shape, 0)
    wave_x = wave_index(row, length) * (2.0 * math.pi / length)
    squared = wave_x * wave_x + wave_y * wave_y
    sign = jnp.where(group < 2, -1.0, 1.0)
    first = params_ref[2 * rows : 2 * rows + 1, 0:LANES]
    second = params_ref[2 * rows + 8 : 2 * rows + 9, 0:LANES]
    base = my_omega(held_ref, surface_ref, tick) * jnp.where(lane < CHUNK, first, second)
    gap = base * base - squared
    fade = jnp.exp(-jnp.sqrt(jnp.maximum(-gap, 0.0)) * depth_step)
    inside = jnp.maximum(gap, 0.0)
    even_ref[...] = fade * polynomial(inside, COS_TERMS)
    odd_ref[...] = sign * (fade * (jnp.sqrt(inside) * polynomial(inside, SIN_TERMS)))


def columns_kernel(*refs, rows, tick):
    in_ref, even_ref, odd_ref, table_ref, flip_ref = refs[:5]
    out_ref = refs[-1]
    table, flipped = Table(table_ref), Table(table_ref, flip_ref)
    length = in_ref.shape[0]
    members = length // rows // GROUPS
    order = [(block % members) * GROUPS + block // members for block in range(length // rows)]
    lane = lax.broadcasted_iota(jnp.int32, (length, LANES), 1)
    low = lane < CHUNK
    turn = jnp.where(low, 1.0, -1.0)
    if tick == 0:
        value = in_ref[:, 0:LANES]
    else:
        value = jnp.concatenate([in_ref[pl.ds(at * rows, rows), :] for at in order], axis=0)
        at_end = lax.axis_index("depth") == lax.axis_size("depth") - 1
        value = jnp.where(at_end, refs[5][:, LANES:], value)
    cos_part, sin_part = analysed_left(flipped, value)
    spectrum = cos_part + turn * pltpu.roll(sin_part, CHUNK, 1)
    swapped = pltpu.roll(spectrum, CHUNK, 1)
    even, odd = even_ref[...], odd_ref[...]
    even_turned, odd_turned = pltpu.roll(even, CHUNK, 1), pltpu.roll(odd, CHUNK, 1)
    shifted = [
        spectrum * jnp.where(low, even, even_turned)
        + swapped * jnp.where(low, -odd, odd_turned),
        spectrum * jnp.where(low, even_turned, even)
        + swapped * jnp.where(low, -odd_turned, odd),
    ]
    cos_part, sin_part = restored_left(table, jnp.concatenate(shifted, axis=1))
    for ref in range(2):
        lanes = slice(ref * LANES, (ref + 1) * LANES)
        result = cos_part[:, lanes] - turn * pltpu.roll(sin_part[:, lanes], CHUNK, 1)
        if tick == 1:
            out_ref[:, lanes] = result
        else:
            for block, at in enumerate(order):
                out_ref[pl.ds(at * rows, rows), lanes] = result[block * rows : (block + 1) * rows]


def inverse_rows(in_ref, table, groups, rows):
    length = in_ref.shape[0] // (groups * rows) * CHUNK
    members = length // CHUNK
    stacked = []
    for ref in range(2):
        lanes = slice(ref * LANES, (ref + 1) * LANES)
        for group in range(groups):
            tiles = []
            for tile in range(length // LANES):
                first = (group * members + 2 * tile) * rows
                tiles.append(
                    swap_halves(
                        in_ref[pl.ds(first, rows), lanes], in_ref[pl.ds(first + rows, rows), lanes]
                    )
                )
            stacked += joined(tiles, 1)
    cos_part, sin_part = restored_right(jnp.concatenate(stacked, axis=0), table)
    results = []
    for ref in range(2):
        for group in range(groups):
            at = (ref * groups + group) * 2 * rows
            real, imag = slice(at, at + rows), slice(at + rows, at + 2 * rows)
            results.append((cos_part[real] - sin_part[imag], cos_part[imag] + sin_part[real]))
    return results[:groups], results[groups:]


def lensed(first, second, weight, lens_cos, lens_sin):
    real = weight * first[0] + (1.0 - weight) * second[0]
    imag = weight * first[1] + (1.0 - weight) * second[1]
    return real * lens_cos - imag * lens_sin, real * lens_sin + imag * lens_cos


def turn_kernel(in_ref, weight_ref, lens_ref, table_ref, flip_ref, *refs, rows):
    out_ref, pieces, field_ref = refs[0], refs[1:5], refs[5]
    held = GROUPS * rows
    first, second = inverse_rows(in_ref, Table(table_ref, flip_ref), 1, held)
    field = lensed(first[0], second[0], weight_ref[...], lens_ref[0], lens_ref[1])
    for part in range(2):
        field_ref[part] = field[part]
    group = my_group()[0]
    for shift in range(GROUPS):
        at = block_row(lax.rem(group + shift, GROUPS), rows)
        for part in range(2):
            pieces[shift][part] = field_ref[part, pl.ds(at, rows), :]
    cos_part, sin_part = analysed_right(jnp.concatenate(field, axis=0), Table(table_ref))
    real, imag = cos_part[:held] + sin_part[held:], cos_part[held:] - sin_part[:held]
    for tile in range(real.shape[1] // LANES):
        lanes = slice(tile * LANES, (tile + 1) * LANES)
        for at, block in enumerate(swap_halves(real[:, lanes], imag[:, lanes])):
            out_ref[pl.ds((2 * tile + at) * held, held), :] = block


def assemble_kernel(*refs, rows):
    pieces, (parts_ref, tail_ref, head_ref) = refs[:GROUPS], refs[GROUPS:]
    group = my_group()[0]
    for shift in range(GROUPS):
        source = lax.rem(group - shift + GROUPS, GROUPS)
        for part in range(2):
            value = pieces[shift][part]
            parts_ref[part * GROUPS + source] = value
            tail_ref[part * GROUPS + source] = value[rows - HALF :]
            head_ref[part * GROUPS + source] = value[:HALF]


def end_kernel(in_ref, lens_ref, params_ref, table_ref, flip_ref, *out_refs, rows):
    parts_ref, tail_ref, head_ref = out_refs
    first, second = inverse_rows(in_ref, Table(table_ref, flip_ref), GROUPS, rows)
    weight = params_ref[pl.ds(rows, rows), :]
    for group in range(GROUPS):
        lens_sin = lens_ref[1, group % 2]
        field = lensed(
            first[group],
            second[group],
            weight,
            lens_ref[0, group % 2],
            lens_sin if group >= 2 else -lens_sin,
        )
        for part in range(2):
            parts_ref[part * GROUPS + group] = field[part]
            tail_ref[part * GROUPS + group] = field[part][rows - HALF :]
            head_ref[part * GROUPS + group] = field[part][:HALF]


def image_body(field_ref, above_ref, below_ref, base_ref, out_ref, padded_ref, rows):
    for index in range(8):
        padded_ref[index, pl.ds(0, HALF)] = above_ref[index]
        padded_ref[index, pl.ds(HALF, rows)] = field_ref[index]
        padded_ref[index, pl.ds(HALF + rows, HALF)] = below_ref[index]
    for lag in range(LAGS):
        offset = lag - HALF
        total = None if base_ref is None else base_ref[lag]
        for part in range(2):
            for freq in range(2):
                source = padded_ref[part * 4 + freq, pl.ds(HALF - offset, rows)]
                receiver = padded_ref[part * 4 + 2 + freq, pl.ds(HALF + offset, rows)]
                total = source * receiver if total is None else total + source * receiver
        out_ref[lag] = total


def image_first(field_ref, above_ref, below_ref, out_ref, padded_ref, *, rows):
    image_body(field_ref, above_ref, below_ref, None, out_ref, padded_ref, rows)


def image_second(field_ref, above_ref, below_ref, base_ref, out_ref, padded_ref, *, rows):
    image_body(field_ref, above_ref, below_ref, base_ref, out_ref, padded_ref, rows)


VMEM = pl.BlockSpec(memory_space=pltpu.VMEM)
SMEM = pl.BlockSpec(memory_space=pltpu.SMEM)


def call(kernel, in_specs, out_shapes, operands, flops, scratch=(), **params):
    many = len(out_shapes) > 1
    shapes = [jax.ShapeDtypeStruct(shape, jnp.float32) for shape in out_shapes]
    return pl.pallas_call(
        functools.partial(kernel, **params),
        in_specs=in_specs,
        out_specs=[VMEM] * len(shapes) if many else VMEM,
        out_shape=shapes if many else shapes[0],
        scratch_shapes=list(scratch),
        cost_estimate=pl.CostEstimate(flops=flops, bytes_accessed=1 << 20, transcendentals=0),
        compiler_params=pltpu.CompilerParams(vmem_limit_bytes=24 << 20),
        interpret=INTERPRET,
    )(*operands)


def shards(
    fields, surface, held_freqs, surface_freqs, ref_slowness, weights, regions, region_slowness
):
    lane_count = lax.axis_size("lat")
    sections = lax.axis_size("depth")
    rows, col_length = fields.shape[4], fields.shape[5]
    length = lane_count * rows
    members = lane_count // GROUPS
    held = GROUPS * rows
    tables_y = transform_tables(col_length)
    tables_x = tables_y if length == col_length else transform_tables(length)
    groups = [[group * members + i for i in range(members)] for group in range(GROUPS)]
    held_freqs = held_freqs[0]

    def exchanged(value, within=None):
        return lax.all_to_all(
            value, "lat", split_axis=0, concat_axis=0, tiled=True, axis_index_groups=within
        )

    def across(pieces):
        moved = [pieces[0]]
        for shift in range(1, GROUPS):
            pairs = [(i, (i + shift * members) % lane_count) for i in range(lane_count)]
            moved.append(lax.ppermute(pieces[shift], "lat", pairs))
        return moved

    def factors(params, tick):
        shape = (length, LANES)
        return call(
            factor_kernel,
            [SMEM, SMEM, VMEM],
            [shape, shape],
            (held_freqs, surface_freqs, params),
            1 << 27,
            tick=tick,
            length=length,
            rows=rows,
        )

    def columns(value, pair, tick, *more):
        return call(
            columns_kernel,
            [VMEM] * (5 + len(more)),
            [(length, 2 * LANES)],
            (value, *pair, *tables_x, *more),
            1 << 29,
            rows=rows,
            tick=tick,
        )

    padded = [pltpu.VMEM((8, rows + 2 * HALF, col_length), jnp.float32)]
    image_shape = (LAGS, rows, col_length)
    parts_shape, edge_shape = (8, rows, col_length), (8, HALF, col_length)
    packed_shape, params_shape = (2 * rows, col_length), (2 * rows + 16, col_length)

    spectra = call(
        rows_kernel,
        [VMEM] * 3,
        [(length, 2 * LANES)],
        (fields.reshape(8 * rows, col_length), surface.reshape(8 * rows, col_length), tables_y[0]),
        1 << 28,
        rows=rows,
    )
    packed, params = call(
        prepare_kernel,
        [VMEM, SMEM, VMEM, SMEM],
        [packed_shape, params_shape],
        (
            regions[0, 0],
            region_slowness[0, 0],
            weights[0, 0],
            ref_slowness[0, 0],
        ),
        1 << 24,
        rows=rows,
    )
    entered = exchanged(spectra)
    packed = across([packed] * GROUPS)
    pair = factors(params, 0)
    shifted = columns(entered, pair, 0)
    returned = exchanged(shifted, groups)
    passed = lax.ppermute(params, "depth", [(s, (s - 1) % sections) for s in range(sections)])
    returned, passed = lax.optimization_barrier((returned, passed))
    weight, lenses = call(
        gather_kernel,
        [SMEM] + [VMEM] * GROUPS,
        [(held, col_length), (2, held, col_length)],
        (held_freqs, *packed),
        1 << 25,
        rows=rows,
    )
    spectra, *pieces = call(
        turn_kernel,
        [VMEM] * 5,
        [(length, LANES)] + [(2, rows, col_length)] * GROUPS,
        (returned, weight, lenses, *tables_y),
        1 << 29,
        [pltpu.VMEM((2, held, col_length), jnp.float32)],
        rows=rows,
    )
    spectra = exchanged(spectra, groups)
    pieces = across(pieces)

    def along(step):
        return [(i, i + step) for i in range(lane_count) if 0 <= i + step < lane_count]

    parts, tail, head = call(
        assemble_kernel,
        [VMEM] * GROUPS,
        [parts_shape, edge_shape, edge_shape],
        pieces,
        1 << 20,
        rows=rows,
    )
    above = lax.ppermute(tail, "lat", along(1))
    below = lax.ppermute(head, "lat", along(-1))
    image = call(
        image_first, [VMEM] * 3, [image_shape], (parts, above, below), 1 << 26, padded, rows=rows
    )
    pair = factors(passed, 1)
    shifted = columns(spectra, pair, 1, entered)
    returned = exchanged(shifted)
    returned, image = lax.optimization_barrier((returned, image))
    lenses = call(
        lens_kernel,
        [SMEM, SMEM, VMEM],
        [(2, 2, rows, col_length)],
        (held_freqs, surface_freqs, passed),
        1 << 24,
        rows=rows,
    )
    parts, tail, head = call(
        end_kernel,
        [VMEM] * 5,
        [parts_shape, edge_shape, edge_shape],
        (returned, lenses, passed, *tables_y),
        1 << 29,
        rows=rows,
    )

    def diagonal(step):
        return [
            (s * lane_count + i, (s + 1) % sections * lane_count + i + step)
            for s in range(sections)
            for i in range(lane_count)
            if 0 <= i + step < lane_count
        ]

    above = lax.ppermute(tail, ("depth", "lat"), diagonal(1))
    below = lax.ppermute(head, ("depth", "lat"), diagonal(-1))
    parts = lax.ppermute(parts, ("depth", "lat"), diagonal(0))
    image = call(
        image_second,
        [VMEM] * 4,
        [image_shape],
        (parts, above, below, image),
        1 << 26,
        padded,
        rows=rows,
    )
    return (parts.reshape(fields.shape), image[None, None])


def solution(mesh):
    in_specs = (
        P("depth", None, None, None, "lat", None),
        P(None, None, None, "lat", None),
        P("depth", None),
        P(),
        P("depth", None, None),
        P("depth", None, "lat", None),
        P("depth", None, "lat", None),
        P("depth", None, None),
    )
    out_specs = (P("depth", None, None, None, "lat", None), P("depth", None, None, "lat", None))

    return jax.shard_map(shards, mesh=mesh, in_specs=in_specs, out_specs=out_specs, check_vma=False)
```

```python
import functools
import math

import jax
import jax.numpy as jnp
import ml_dtypes
import numpy as np
from jax import lax
from jax.experimental import pallas as pl
from jax.experimental.pallas import tpu as pltpu
from jax.sharding import PartitionSpec as P

LAGS = 16
HALF = LAGS // 2
REGIONS = 8
GROUPS = 4
CHUNK = 64
LANES = 128
INTERPRET = False

omega_step = 0.04
depth_step = 1.0

COS_TERMS = [(-1.0) ** n / math.factorial(2 * n) for n in range(12)]
SIN_TERMS = [(-1.0) ** n / math.factorial(2 * n + 1) for n in range(12)]


def polynomial(value, terms):
    total = jnp.full_like(value, terms[-1])
    for term in terms[-2::-1]:
        total = total * value + term
    return total


def transform_tables(length):
    half = length // 2
    index = np.arange(half)
    even = 2.0 * np.pi * (2 * index[:, None] * index[None, :] % length) / length
    odd = 2.0 * np.pi * (index[:, None] * (2 * index[None, :] + 1) % length) / length
    tables = []
    for angles in ([even, odd], [odd.T]):
        table = np.concatenate([f(a) for a in angles for f in (np.cos, np.sin)], axis=1)
        lead = table.astype(ml_dtypes.bfloat16)
        trail = (table - lead.astype(np.float64)).astype(ml_dtypes.bfloat16)
        tables.append(jnp.asarray(np.concatenate([lead, trail], axis=1)))
    return tables


class Table:
    def __init__(self, main_ref, odd_ref=None):
        self.main, self.odd = main_ref, odd_ref
        self.width = main_ref.shape[0]

    def part(self, part, first, count, trail):
        if part == 1 and self.odd is not None:
            start = (2 * trail + first) * self.width
            return self.odd[:, start : start + count * self.width]
        start = (4 * trail + 2 * part + first) * self.width
        return self.main[:, start : start + count * self.width]


def two_parts(value):
    lead = value.astype(jnp.bfloat16)
    return lead, (value - lead.astype(jnp.float32)).astype(jnp.bfloat16)


def dot(left, right):
    return jnp.dot(left, right, preferred_element_type=jnp.float32)


def dot_right(value, table, part):
    width = value.shape[1]
    lead, trail = two_parts(value)
    main, rest = table.part(part, 0, 2, 0), table.part(part, 0, 2, 1)
    both = dot(lead, main) + (dot(trail, main) + dot(lead, rest))
    return both[:, :width], both[:, width:]


def dot_left(table, part, value):
    lead, trail = two_parts(value)
    results = []
    for which in range(2):
        main, rest = table.part(part, which, 1, 0), table.part(part, which, 1, 1)
        results.append(dot(main, lead) + (dot(main, trail) + dot(rest, lead)))
    return results


def joined(pairs, axis):
    return [jnp.concatenate([pair[i] for pair in pairs], axis=axis) for i in range(2)]


def analysed_right(value, table):
    half = value.shape[1] // 2
    low, high = value[:, :half], value[:, half:]
    return joined([dot_right(low + high, table, 0), dot_right(low - high, table, 1)], 1)


def restored_right(value, table):
    half = value.shape[1] // 2
    even, odd = dot_right(value[:, :half], table, 0), dot_right(value[:, half:], table, 1)
    return joined([[e + o for e, o in zip(even, odd)], [e - o for e, o in zip(even, odd)]], 1)


def analysed_left(table, value):
    half = value.shape[0] // 2
    low, high = value[:half], value[half:]
    return joined([dot_left(table, 0, low + high), dot_left(table, 1, low - high)], 0)


def restored_left(table, value):
    half = value.shape[0] // 2
    even, odd = dot_left(table, 0, value[:half]), dot_left(table, 1, value[half:])
    return joined([[e + o for e, o in zip(even, odd)], [e - o for e, o in zip(even, odd)]], 0)


def swap_halves(first, second):
    lane = lax.broadcasted_iota(jnp.int32, first.shape, 1)
    low = lane < CHUNK
    return (
        jnp.where(low, first, pltpu.roll(second, CHUNK, 1)),
        jnp.where(low, pltpu.roll(first, CHUNK, 1), second),
    )


def wave_index(position, length):
    half = length // 2
    index = jnp.where(position < half, 2 * position, 2 * (position - half) + 1)
    return jnp.where(index < half, index, index - length).astype(jnp.float32)


def block_row(index, rows):
    return pl.multiple_of(index * rows, rows)


def my_group():
    lat = lax.axis_index("lat")
    members = lax.axis_size("lat") // GROUPS
    return lax.div(lat, members), lax.rem(lat, members)


def omega_pair(held_ref, surface_ref, tick):
    pair = []
    for freq in range(2):
        number = held_ref[freq]
        if tick == 1:
            at_end = lax.axis_index("depth") == lax.axis_size("depth") - 1
            number = jnp.where(at_end, surface_ref[freq], number)
        pair.append(number.astype(jnp.float32) * omega_step)
    return pair


def my_omega(held_ref, surface_ref, tick):
    pair = omega_pair(held_ref, surface_ref, tick)
    return jnp.where(lax.rem(my_group()[0], 2) == 0, pair[0], pair[1])


def lens(angle, scale):
    square = angle * angle
    return (
        polynomial(square, COS_TERMS) * scale,
        angle * polynomial(square, SIN_TERMS) * scale,
    )


def prepare_kernel(
    regions_ref, region_slow_ref, weights_ref, slow_ref, packed_ref, params_ref, *, rows
):
    regions, weight = regions_ref[...], weights_ref[...]
    cell = jnp.full(weight.shape, region_slow_ref[0])
    for region in range(1, REGIONS):
        cell = jnp.where(regions == region, region_slow_ref[region], cell)
    gap = cell - (weight * slow_ref[0] + (1.0 - weight) * slow_ref[1])
    for out in (packed_ref, params_ref):
        out[pl.ds(0, rows), :] = gap
        out[pl.ds(rows, rows), :] = weight
    for ref in range(2):
        params_ref[pl.ds(2 * rows + 8 * ref, 8), :] = jnp.full((8, weight.shape[1]), slow_ref[ref])


def gather_kernel(held_ref, *refs, rows):
    pieces, (weight_ref, lens_ref) = refs[:GROUPS], refs[GROUPS:]
    group = my_group()[0]
    omega = my_omega(held_ref, None, 0)
    sign = jnp.where(group < 2, -1.0, 1.0)
    scale = 1.0 / (weight_ref.shape[1] * (lax.axis_size("lat") * rows))
    for shift in range(GROUPS):
        piece = pieces[shift]
        source = lax.rem(group - shift + GROUPS, GROUPS)
        at = block_row(source, rows)
        weight_ref[pl.ds(at, rows), :] = piece[pl.ds(rows, rows), :]
        cos_part, sin_part = lens(piece[pl.ds(0, rows), :] * omega * depth_step, scale)
        lens_ref[0, pl.ds(at, rows), :] = cos_part
        lens_ref[1, pl.ds(at, rows), :] = sin_part * sign


def lens_kernel(held_ref, surface_freq_ref, passed_ref, lens_ref, *, rows):
    scale = 1.0 / (passed_ref.shape[1] * (lax.axis_size("lat") * rows))
    for freq, omega in enumerate(omega_pair(held_ref, surface_freq_ref, 1)):
        cos_part, sin_part = lens(passed_ref[pl.ds(0, rows), :] * omega * depth_step, scale)
        lens_ref[0, freq] = cos_part
        lens_ref[1, freq] = sin_part


def rows_kernel(field_ref, surface_ref, table_ref, out_ref, *, rows):
    half = field_ref.shape[0] // 2
    members = field_ref.shape[1] // CHUNK
    value = jnp.concatenate([field_ref[...], surface_ref[...]], axis=0)
    cos_part, sin_part = analysed_right(value, Table(table_ref))
    for batch in range(2):
        at_real = 2 * half * batch
        at_imag = at_real + half
        real = cos_part[at_real:at_imag] + sin_part[at_imag : at_imag + half]
        imag = cos_part[at_imag : at_imag + half] - sin_part[at_real:at_imag]
        out_lanes = slice(batch * LANES, (batch + 1) * LANES)
        for tile in range(field_ref.shape[1] // LANES):
            lanes = slice(tile * LANES, (tile + 1) * LANES)
            for at, block in enumerate(swap_halves(real[:, lanes], imag[:, lanes])):
                for group in range(GROUPS):
                    start = (group * members + 2 * tile + at) * rows
                    out_ref[pl.ds(start, rows), out_lanes] = block[group * rows : (group + 1) * rows]


def factor_kernel(held_ref, surface_ref, params_ref, even_ref, odd_ref, *, tick, length, rows):
    col_length = params_ref.shape[1]
    shape = (length, LANES)
    lane = lax.broadcasted_iota(jnp.int32, (1, LANES), 1)
    group, member = my_group()
    wave_y = wave_index(member * CHUNK + lax.rem(lane, CHUNK), col_length) * (
        2.0 * math.pi / col_length
    )
    row = lax.broadcasted_iota(jnp.int32, shape, 0)
    wave_x = wave_index(row, length) * (2.0 * math.pi / length)
    squared = wave_x * wave_x + wave_y * wave_y
    sign = jnp.where(group < 2, -1.0, 1.0)
    first = params_ref[2 * rows : 2 * rows + 1, 0:LANES]
    second = params_ref[2 * rows + 8 : 2 * rows + 9, 0:LANES]
    base = my_omega(held_ref, surface_ref, tick) * jnp.where(lane < CHUNK, first, second)
    gap = base * base - squared
    fade = jnp.exp(-jnp.sqrt(jnp.maximum(-gap, 0.0)) * depth_step)
    inside = jnp.maximum(gap, 0.0)
    even_ref[...] = fade * polynomial(inside, COS_TERMS)
    odd_ref[...] = sign * (fade * (jnp.sqrt(inside) * polynomial(inside, SIN_TERMS)))


def columns_kernel(*refs, rows, tick):
    in_ref, even_ref, odd_ref, table_ref, flip_ref = refs[:5]
    out_ref = refs[5] if tick == 0 else refs[6]
    table, flipped = Table(table_ref), Table(table_ref, flip_ref)
    length = in_ref.shape[0]
    members = length // rows // GROUPS
    order = [(block % members) * GROUPS + block // members for block in range(length // rows)]
    lane = lax.broadcasted_iota(jnp.int32, (length, LANES), 1)
    low = lane < CHUNK
    turn = jnp.where(low, 1.0, -1.0)
    if tick == 0:
        value = in_ref[:, 0:LANES]
        refs[6][...] = in_ref[:, LANES:]
    else:
        value = jnp.concatenate([in_ref[pl.ds(at * rows, rows), :] for at in order], axis=0)
        at_end = lax.axis_index("depth") == lax.axis_size("depth") - 1
        value = jnp.where(at_end, refs[5][...], value)
    cos_part, sin_part = analysed_left(flipped, value)
    spectrum = cos_part + turn * pltpu.roll(sin_part, CHUNK, 1)
    swapped = pltpu.roll(spectrum, CHUNK, 1)
    even, odd = even_ref[...], odd_ref[...]
    even_turned, odd_turned = pltpu.roll(even, CHUNK, 1), pltpu.roll(odd, CHUNK, 1)
    shifted = [
        spectrum * jnp.where(low, even, even_turned)
        + swapped * jnp.where(low, -odd, odd_turned),
        spectrum * jnp.where(low, even_turned, even)
        + swapped * jnp.where(low, -odd_turned, odd),
    ]
    cos_part, sin_part = restored_left(table, jnp.concatenate(shifted, axis=1))
    for ref in range(2):
        lanes = slice(ref * LANES, (ref + 1) * LANES)
        result = cos_part[:, lanes] - turn * pltpu.roll(sin_part[:, lanes], CHUNK, 1)
        if tick == 1:
            out_ref[:, lanes] = result
        else:
            for block, at in enumerate(order):
                out_ref[pl.ds(at * rows, rows), lanes] = result[block * rows : (block + 1) * rows]


def inverse_rows(in_ref, table, groups, rows):
    length = in_ref.shape[0] // (groups * rows) * CHUNK
    members = length // CHUNK
    stacked = []
    for ref in range(2):
        lanes = slice(ref * LANES, (ref + 1) * LANES)
        for group in range(groups):
            tiles = []
            for tile in range(length // LANES):
                first = (group * members + 2 * tile) * rows
                tiles.append(
                    swap_halves(
                        in_ref[pl.ds(first, rows), lanes], in_ref[pl.ds(first + rows, rows), lanes]
                    )
                )
            stacked += joined(tiles, 1)
    cos_part, sin_part = restored_right(jnp.concatenate(stacked, axis=0), table)
    results = []
    for ref in range(2):
        for group in range(groups):
            at = (ref * groups + group) * 2 * rows
            real, imag = slice(at, at + rows), slice(at + rows, at + 2 * rows)
            results.append((cos_part[real] - sin_part[imag], cos_part[imag] + sin_part[real]))
    return results[:groups], results[groups:]


def lensed(first, second, weight, lens_cos, lens_sin):
    real = weight * first[0] + (1.0 - weight) * second[0]
    imag = weight * first[1] + (1.0 - weight) * second[1]
    return real * lens_cos - imag * lens_sin, real * lens_sin + imag * lens_cos


def turn_kernel(in_ref, weight_ref, lens_ref, table_ref, flip_ref, *refs, rows):
    out_ref, pieces, field_ref = refs[0], refs[1:5], refs[5]
    held = GROUPS * rows
    first, second = inverse_rows(in_ref, Table(table_ref, flip_ref), 1, held)
    field = lensed(first[0], second[0], weight_ref[...], lens_ref[0], lens_ref[1])
    for part in range(2):
        field_ref[part] = field[part]
    group = my_group()[0]
    for shift in range(GROUPS):
        at = block_row(lax.rem(group + shift, GROUPS), rows)
        for part in range(2):
            pieces[shift][part] = field_ref[part, pl.ds(at, rows), :]
    cos_part, sin_part = analysed_right(jnp.concatenate(field, axis=0), Table(table_ref))
    real, imag = cos_part[:held] + sin_part[held:], cos_part[held:] - sin_part[:held]
    for tile in range(real.shape[1] // LANES):
        lanes = slice(tile * LANES, (tile + 1) * LANES)
        for at, block in enumerate(swap_halves(real[:, lanes], imag[:, lanes])):
            out_ref[pl.ds((2 * tile + at) * held, held), :] = block


def assemble_kernel(*refs, rows):
    pieces, (parts_ref, tail_ref, head_ref) = refs[:GROUPS], refs[GROUPS:]
    group = my_group()[0]
    for shift in range(GROUPS):
        source = lax.rem(group - shift + GROUPS, GROUPS)
        for part in range(2):
            value = pieces[shift][part]
            parts_ref[part * GROUPS + source] = value
            tail_ref[part * GROUPS + source] = value[rows - HALF :]
            head_ref[part * GROUPS + source] = value[:HALF]


def end_kernel(in_ref, lens_ref, params_ref, table_ref, flip_ref, *out_refs, rows):
    parts_ref, tail_ref, head_ref = out_refs
    first, second = inverse_rows(in_ref, Table(table_ref, flip_ref), GROUPS, rows)
    weight = params_ref[pl.ds(rows, rows), :]
    for group in range(GROUPS):
        lens_sin = lens_ref[1, group % 2]
        field = lensed(
            first[group],
            second[group],
            weight,
            lens_ref[0, group % 2],
            lens_sin if group >= 2 else -lens_sin,
        )
        for part in range(2):
            parts_ref[part * GROUPS + group] = field[part]
            tail_ref[part * GROUPS + group] = field[part][rows - HALF :]
            head_ref[part * GROUPS + group] = field[part][:HALF]


def image_body(field_ref, above_ref, below_ref, base_ref, out_ref, padded_ref, rows):
    for index in range(8):
        padded_ref[index, pl.ds(0, HALF)] = above_ref[index]
        padded_ref[index, pl.ds(HALF, rows)] = field_ref[index]
        padded_ref[index, pl.ds(HALF + rows, HALF)] = below_ref[index]
    for lag in range(LAGS):
        offset = lag - HALF
        total = None if base_ref is None else base_ref[lag]
        for part in range(2):
            for freq in range(2):
                source = padded_ref[part * 4 + freq, pl.ds(HALF - offset, rows)]
                receiver = padded_ref[part * 4 + 2 + freq, pl.ds(HALF + offset, rows)]
                total = source * receiver if total is None else total + source * receiver
        out_ref[lag] = total


def image_first(field_ref, above_ref, below_ref, out_ref, padded_ref, *, rows):
    image_body(field_ref, above_ref, below_ref, None, out_ref, padded_ref, rows)


def image_second(field_ref, above_ref, below_ref, base_ref, out_ref, padded_ref, *, rows):
    image_body(field_ref, above_ref, below_ref, base_ref, out_ref, padded_ref, rows)


def store_kernel(in_ref, out_ref):
    out_ref[...] = in_ref[...]


VMEM = pl.BlockSpec(memory_space=pltpu.VMEM)
SMEM = pl.BlockSpec(memory_space=pltpu.SMEM)


def call(kernel, in_specs, out_shapes, operands, flops, scratch=(), **params):
    many = len(out_shapes) > 1
    shapes = [jax.ShapeDtypeStruct(shape, jnp.float32) for shape in out_shapes]
    return pl.pallas_call(
        functools.partial(kernel, **params),
        in_specs=in_specs,
        out_specs=[VMEM] * len(shapes) if many else VMEM,
        out_shape=shapes if many else shapes[0],
        scratch_shapes=list(scratch),
        cost_estimate=pl.CostEstimate(flops=flops, bytes_accessed=1 << 20, transcendentals=0),
        compiler_params=pltpu.CompilerParams(vmem_limit_bytes=24 << 20),
        interpret=INTERPRET,
    )(*operands)


def shards(
    fields, surface, held_freqs, surface_freqs, ref_slowness, weights, regions, region_slowness
):
    lane_count = lax.axis_size("lat")
    sections = lax.axis_size("depth")
    rows, col_length = fields.shape[4], fields.shape[5]
    length = lane_count * rows
    members = lane_count // GROUPS
    held = GROUPS * rows
    tables_y = transform_tables(col_length)
    tables_x = tables_y if length == col_length else transform_tables(length)
    groups = [[group * members + i for i in range(members)] for group in range(GROUPS)]
    held_freqs = held_freqs[0]

    def exchanged(value, within=None):
        return lax.all_to_all(
            value, "lat", split_axis=0, concat_axis=0, tiled=True, axis_index_groups=within
        )

    def across(pieces):
        moved = [pieces[0]]
        for shift in range(1, GROUPS):
            pairs = [(i, (i + shift * members) % lane_count) for i in range(lane_count)]
            moved.append(lax.ppermute(pieces[shift], "lat", pairs))
        return moved

    def factors(params, tick):
        shape = (length, LANES)
        return call(
            factor_kernel,
            [SMEM, SMEM, VMEM],
            [shape, shape],
            (held_freqs, surface_freqs, params),
            1 << 27,
            tick=tick,
            length=length,
            rows=rows,
        )

    def columns(value, pair, tick, *more):
        return call(
            columns_kernel,
            [VMEM] * (5 + len(more)),
            [(length, 2 * LANES)] + [(length, LANES)] * (1 - tick),
            (value, *pair, *tables_x, *more),
            1 << 29,
            rows=rows,
            tick=tick,
        )

    padded = [pltpu.VMEM((8, rows + 2 * HALF, col_length), jnp.float32)]
    image_shape = (LAGS, rows, col_length)
    parts_shape, edge_shape = (8, rows, col_length), (8, HALF, col_length)
    packed_shape, params_shape = (2 * rows, col_length), (2 * rows + 16, col_length)

    spectra = call(
        rows_kernel,
        [VMEM] * 3,
        [(length, 2 * LANES)],
        (fields.reshape(8 * rows, col_length), surface.reshape(8 * rows, col_length), tables_y[0]),
        1 << 28,
        rows=rows,
    )
    packed, params = call(
        prepare_kernel,
        [VMEM, SMEM, VMEM, SMEM],
        [packed_shape, params_shape],
        (
            regions[0, 0],
            region_slowness[0, 0],
            weights[0, 0],
            ref_slowness[0, 0],
        ),
        1 << 24,
        rows=rows,
    )
    entered = exchanged(spectra)
    packed = across([packed] * GROUPS)
    pair = factors(params, 0)
    shifted, later = columns(entered, pair, 0)
    returned = exchanged(shifted, groups)
    upward = [(s, (s - 1) % sections) for s in range(sections)]
    passed = lax.ppermute(params, "depth", upward)
    weight, lenses = call(
        gather_kernel,
        [SMEM] + [VMEM] * GROUPS,
        [(held, col_length), (2, held, col_length)],
        (held_freqs, *packed),
        1 << 25,
        rows=rows,
    )
    next_pair = factors(passed, 1)
    spectra, *pieces = call(
        turn_kernel,
        [VMEM] * 5,
        [(length, LANES)] + [(2, rows, col_length)] * GROUPS,
        (returned, weight, lenses, *tables_y),
        1 << 29,
        [pltpu.VMEM((2, held, col_length), jnp.float32)],
        rows=rows,
    )
    spectra = exchanged(spectra, groups)
    pieces = across(pieces)

    def along(step):
        return [(i, i + step) for i in range(lane_count) if 0 <= i + step < lane_count]

    parts, tail, head = call(
        assemble_kernel,
        [VMEM] * GROUPS,
        [parts_shape, edge_shape, edge_shape],
        pieces,
        1 << 20,
        rows=rows,
    )
    above = lax.ppermute(tail, "lat", along(1))
    below = lax.ppermute(head, "lat", along(-1))
    image = call(
        image_first, [VMEM] * 3, [image_shape], (parts, above, below), 1 << 26, padded, rows=rows
    )
    shifted = columns(spectra, next_pair, 1, later)
    returned = exchanged(shifted)
    lenses = call(
        lens_kernel,
        [SMEM, SMEM, VMEM],
        [(2, 2, rows, col_length)],
        (held_freqs, surface_freqs, passed),
        1 << 24,
        rows=rows,
    )
    parts, tail, head = call(
        end_kernel,
        [VMEM] * 5,
        [parts_shape, edge_shape, edge_shape],
        (returned, lenses, passed, *tables_y),
        1 << 29,
        rows=rows,
    )

    def diagonal(step):
        return [
            (s * lane_count + i, (s + 1) % sections * lane_count + i + step)
            for s in range(sections)
            for i in range(lane_count)
            if 0 <= i + step < lane_count
        ]

    above = lax.ppermute(tail, ("depth", "lat"), diagonal(1))
    below = lax.ppermute(head, ("depth", "lat"), diagonal(-1))
    parts = lax.ppermute(parts, ("depth", "lat"), diagonal(0))
    image = call(
        image_second,
        [VMEM] * 4,
        [image_shape],
        (parts, above, below, image),
        1 << 26,
        padded,
        rows=rows,
    )
    stored = call(store_kernel, [VMEM], [parts_shape], (parts,), 1 << 20)
    return (stored.reshape(fields.shape), image[None, None])


def solution(mesh):
    in_specs = (
        P("depth", None, None, None, "lat", None),
        P(None, None, None, "lat", None),
        P("depth", None),
        P(),
        P("depth", None, None),
        P("depth", None, "lat", None),
        P("depth", None, "lat", None),
        P("depth", None, None),
    )
    out_specs = (P("depth", None, None, None, "lat", None), P("depth", None, None, "lat", None))


    return jax.shard_map(shards, mesh=mesh, in_specs=in_specs, out_specs=out_specs, check_vma=False)
```

```python
import functools
import math

import jax
import jax.numpy as jnp
import ml_dtypes
import numpy as np
from jax import lax
from jax.experimental import pallas as pl
from jax.experimental.pallas import tpu as pltpu
from jax.sharding import PartitionSpec as P

LAGS = 16
HALF = LAGS // 2
REGIONS = 8
GROUPS = 4
CHUNK = 64
LANES = 128
INTERPRET = False

omega_step = 0.04
depth_step = 1.0

COS_TERMS = [(-1.0) ** n / math.factorial(2 * n) for n in range(12)]
SIN_TERMS = [(-1.0) ** n / math.factorial(2 * n + 1) for n in range(12)]


def polynomial(value, terms):
    total = jnp.full_like(value, terms[-1])
    for term in terms[-2::-1]:
        total = total * value + term
    return total


def transform_tables(length):
    half = length // 2
    index = np.arange(half)
    even = 2.0 * np.pi * (2 * index[:, None] * index[None, :] % length) / length
    odd = 2.0 * np.pi * (index[:, None] * (2 * index[None, :] + 1) % length) / length
    tables = []
    for angles in ([even, odd], [odd.T]):
        table = np.concatenate([f(a) for a in angles for f in (np.cos, np.sin)], axis=1)
        lead = table.astype(ml_dtypes.bfloat16)
        trail = (table - lead.astype(np.float64)).astype(ml_dtypes.bfloat16)
        tables.append(jnp.asarray(np.concatenate([lead, trail], axis=1)))
    return tables


class Table:
    def __init__(self, main_ref, odd_ref=None):
        self.main, self.odd = main_ref, odd_ref
        self.width = main_ref.shape[0]

    def part(self, part, first, count, trail):
        if part == 1 and self.odd is not None:
            start = (2 * trail + first) * self.width
            return self.odd[:, start : start + count * self.width]
        start = (4 * trail + 2 * part + first) * self.width
        return self.main[:, start : start + count * self.width]


def two_parts(value):
    lead = value.astype(jnp.bfloat16)
    return lead, (value - lead.astype(jnp.float32)).astype(jnp.bfloat16)


def dot(left, right):
    return jnp.dot(left, right, preferred_element_type=jnp.float32)


def dot_right(value, table, part):
    width = value.shape[1]
    lead, trail = two_parts(value)
    main, rest = table.part(part, 0, 2, 0), table.part(part, 0, 2, 1)
    both = dot(lead, main) + (dot(trail, main) + dot(lead, rest))
    return both[:, :width], both[:, width:]


def dot_left(table, part, value):
    lead, trail = two_parts(value)
    results = []
    for which in range(2):
        main, rest = table.part(part, which, 1, 0), table.part(part, which, 1, 1)
        results.append(dot(main, lead) + (dot(main, trail) + dot(rest, lead)))
    return results


def joined(pairs, axis):
    return [jnp.concatenate([pair[i] for pair in pairs], axis=axis) for i in range(2)]


def analysed_right(value, table):
    half = value.shape[1] // 2
    low, high = value[:, :half], value[:, half:]
    return joined([dot_right(low + high, table, 0), dot_right(low - high, table, 1)], 1)


def restored_right(value, table):
    half = value.shape[1] // 2
    even, odd = dot_right(value[:, :half], table, 0), dot_right(value[:, half:], table, 1)
    return joined([[e + o for e, o in zip(even, odd)], [e - o for e, o in zip(even, odd)]], 1)


def analysed_left(table, value):
    half = value.shape[0] // 2
    low, high = value[:half], value[half:]
    return joined([dot_left(table, 0, low + high), dot_left(table, 1, low - high)], 0)


def restored_left(table, value):
    half = value.shape[0] // 2
    even, odd = dot_left(table, 0, value[:half]), dot_left(table, 1, value[half:])
    return joined([[e + o for e, o in zip(even, odd)], [e - o for e, o in zip(even, odd)]], 0)


def swap_halves(first, second):
    lane = lax.broadcasted_iota(jnp.int32, first.shape, 1)
    low = lane < CHUNK
    return (
        jnp.where(low, first, pltpu.roll(second, CHUNK, 1)),
        jnp.where(low, pltpu.roll(first, CHUNK, 1), second),
    )


def wave_index(position, length):
    half = length // 2
    index = jnp.where(position < half, 2 * position, 2 * (position - half) + 1)
    return jnp.where(index < half, index, index - length).astype(jnp.float32)


def block_row(index, rows):
    return pl.multiple_of(index * rows, rows)


def my_group():
    lat = lax.axis_index("lat")
    members = lax.axis_size("lat") // GROUPS
    return lax.div(lat, members), lax.rem(lat, members)


def omega_pair(held_ref, surface_ref, tick):
    pair = []
    for freq in range(2):
        number = held_ref[freq]
        if tick == 1:
            at_end = lax.axis_index("depth") == lax.axis_size("depth") - 1
            number = jnp.where(at_end, surface_ref[freq], number)
        pair.append(number.astype(jnp.float32) * omega_step)
    return pair


def my_omega(held_ref, surface_ref, tick):
    pair = omega_pair(held_ref, surface_ref, tick)
    return jnp.where(lax.rem(my_group()[0], 2) == 0, pair[0], pair[1])


def lens(angle, scale):
    square = angle * angle
    return (
        polynomial(square, COS_TERMS) * scale,
        angle * polynomial(square, SIN_TERMS) * scale,
    )


def prepare_kernel(
    regions_ref, region_slow_ref, weights_ref, slow_ref, surface_ref, *out_refs, rows
):
    regions, weight = regions_ref[...], weights_ref[...]
    cell = jnp.full(weight.shape, region_slow_ref[0])
    for region in range(1, REGIONS):
        cell = jnp.where(regions == region, region_slow_ref[region], cell)
    gap = cell - (weight * slow_ref[0] + (1.0 - weight) * slow_ref[1])
    params_ref = out_refs[GROUPS]
    group = my_group()[0]
    for shift in range(GROUPS):
        sent = lax.rem(group + shift, GROUPS)
        for part in range(2):
            at = pl.ds((2 + part) * rows, rows)
            out_refs[shift][at, :] = surface_ref[part * GROUPS + sent]
    for out in out_refs:
        out[pl.ds(0, rows), :] = gap
        out[pl.ds(rows, rows), :] = weight
    for ref in range(2):
        params_ref[pl.ds(2 * rows + 8 * ref, 8), :] = jnp.full((8, weight.shape[1]), slow_ref[ref])


def gather_kernel(held_ref, *refs, rows):
    pieces, (weight_ref, lens_ref, surface_ref) = refs[:GROUPS], refs[GROUPS:]
    group = my_group()[0]
    omega = my_omega(held_ref, None, 0)
    sign = jnp.where(group < 2, -1.0, 1.0)
    scale = 1.0 / (weight_ref.shape[1] * (lax.axis_size("lat") * rows))
    for shift in range(GROUPS):
        piece = pieces[shift]
        source = lax.rem(group - shift + GROUPS, GROUPS)
        at = block_row(source, rows)
        weight_ref[pl.ds(at, rows), :] = piece[pl.ds(rows, rows), :]
        cos_part, sin_part = lens(piece[pl.ds(0, rows), :] * omega * depth_step, scale)
        lens_ref[0, pl.ds(at, rows), :] = cos_part
        lens_ref[1, pl.ds(at, rows), :] = sin_part * sign
        for part in range(2):
            surface_ref[part, pl.ds(at, rows), :] = piece[pl.ds((2 + part) * rows, rows), :]


def lens_kernel(held_ref, surface_freq_ref, passed_ref, lens_ref, *, rows):
    scale = 1.0 / (passed_ref.shape[1] * (lax.axis_size("lat") * rows))
    for freq, omega in enumerate(omega_pair(held_ref, surface_freq_ref, 1)):
        cos_part, sin_part = lens(passed_ref[pl.ds(0, rows), :] * omega * depth_step, scale)
        lens_ref[0, freq] = cos_part
        lens_ref[1, freq] = sin_part


def rows_kernel(field_ref, table_ref, out_ref, *, rows):
    half = field_ref.shape[0] // 2
    members = field_ref.shape[1] // CHUNK
    cos_part, sin_part = analysed_right(field_ref[...], Table(table_ref))
    real, imag = cos_part[:half] + sin_part[half:], cos_part[half:] - sin_part[:half]
    for tile in range(field_ref.shape[1] // LANES):
        lanes = slice(tile * LANES, (tile + 1) * LANES)
        for at, block in enumerate(swap_halves(real[:, lanes], imag[:, lanes])):
            for group in range(GROUPS):
                start = (group * members + 2 * tile + at) * rows
                out_ref[pl.ds(start, rows), :] = block[group * rows : (group + 1) * rows]


def factor_kernel(held_ref, surface_ref, params_ref, even_ref, odd_ref, *, tick, length, rows):
    col_length = params_ref.shape[1]
    shape = (length, LANES)
    lane = lax.broadcasted_iota(jnp.int32, (1, LANES), 1)
    group, member = my_group()
    wave_y = wave_index(member * CHUNK + lax.rem(lane, CHUNK), col_length) * (
        2.0 * math.pi / col_length
    )
    row = lax.broadcasted_iota(jnp.int32, shape, 0)
    wave_x = wave_index(row, length) * (2.0 * math.pi / length)
    squared = wave_x * wave_x + wave_y * wave_y
    sign = jnp.where(group < 2, -1.0, 1.0)
    first = params_ref[2 * rows : 2 * rows + 1, 0:LANES]
    second = params_ref[2 * rows + 8 : 2 * rows + 9, 0:LANES]
    base = my_omega(held_ref, surface_ref, tick) * jnp.where(lane < CHUNK, first, second)
    gap = base * base - squared
    fade = jnp.exp(-jnp.sqrt(jnp.maximum(-gap, 0.0)) * depth_step)
    inside = jnp.maximum(gap, 0.0)
    even_ref[...] = fade * polynomial(inside, COS_TERMS)
    odd_ref[...] = sign * (fade * (jnp.sqrt(inside) * polynomial(inside, SIN_TERMS)))


def columns_kernel(*refs, rows, tick):
    in_ref, even_ref, odd_ref, table_ref, flip_ref = refs[:5]
    out_ref = refs[5]
    table, flipped = Table(table_ref), Table(table_ref, flip_ref)
    length = in_ref.shape[0]
    members = length // rows // GROUPS
    order = [(block % members) * GROUPS + block // members for block in range(length // rows)]
    lane = lax.broadcasted_iota(jnp.int32, (length, LANES), 1)
    low = lane < CHUNK
    turn = jnp.where(low, 1.0, -1.0)
    if tick == 0:
        value = in_ref[...]
    else:
        value = jnp.concatenate([in_ref[pl.ds(at * rows, rows), :] for at in order], axis=0)
    cos_part, sin_part = analysed_left(flipped, value)
    spectrum = cos_part + turn * pltpu.roll(sin_part, CHUNK, 1)
    swapped = pltpu.roll(spectrum, CHUNK, 1)
    even, odd = even_ref[...], odd_ref[...]
    even_turned, odd_turned = pltpu.roll(even, CHUNK, 1), pltpu.roll(odd, CHUNK, 1)
    shifted = [
        spectrum * jnp.where(low, even, even_turned)
        + swapped * jnp.where(low, -odd, odd_turned),
        spectrum * jnp.where(low, even_turned, even)
        + swapped * jnp.where(low, -odd_turned, odd),
    ]
    cos_part, sin_part = restored_left(table, jnp.concatenate(shifted, axis=1))
    for ref in range(2):
        lanes = slice(ref * LANES, (ref + 1) * LANES)
        result = cos_part[:, lanes] - turn * pltpu.roll(sin_part[:, lanes], CHUNK, 1)
        if tick == 1:
            out_ref[:, lanes] = result
        else:
            for block, at in enumerate(order):
                out_ref[pl.ds(at * rows, rows), lanes] = result[block * rows : (block + 1) * rows]


def inverse_rows(in_ref, table, groups, rows):
    length = in_ref.shape[0] // (groups * rows) * CHUNK
    members = length // CHUNK
    stacked = []
    for ref in range(2):
        lanes = slice(ref * LANES, (ref + 1) * LANES)
        for group in range(groups):
            tiles = []
            for tile in range(length // LANES):
                first = (group * members + 2 * tile) * rows
                tiles.append(
                    swap_halves(
                        in_ref[pl.ds(first, rows), lanes], in_ref[pl.ds(first + rows, rows), lanes]
                    )
                )
            stacked += joined(tiles, 1)
    cos_part, sin_part = restored_right(jnp.concatenate(stacked, axis=0), table)
    results = []
    for ref in range(2):
        for group in range(groups):
            at = (ref * groups + group) * 2 * rows
            real, imag = slice(at, at + rows), slice(at + rows, at + 2 * rows)
            results.append((cos_part[real] - sin_part[imag], cos_part[imag] + sin_part[real]))
    return results[:groups], results[groups:]


def lensed(first, second, weight, lens_cos, lens_sin):
    real = weight * first[0] + (1.0 - weight) * second[0]
    imag = weight * first[1] + (1.0 - weight) * second[1]
    return real * lens_cos - imag * lens_sin, real * lens_sin + imag * lens_cos


def turn_kernel(in_ref, weight_ref, lens_ref, surface_ref, table_ref, flip_ref, *refs, rows):
    out_ref, pieces, field_ref = refs[0], refs[1:5], refs[5]
    held = GROUPS * rows
    first, second = inverse_rows(in_ref, Table(table_ref, flip_ref), 1, held)
    field = lensed(first[0], second[0], weight_ref[...], lens_ref[0], lens_ref[1])
    at_end = lax.axis_index("depth") == lax.axis_size("depth") - 1
    start = []
    for part in range(2):
        field_ref[part] = field[part]
        start.append(jnp.where(at_end, surface_ref[part], field[part]))
    group = my_group()[0]
    for shift in range(GROUPS):
        at = block_row(lax.rem(group + shift, GROUPS), rows)
        for part in range(2):
            pieces[shift][part] = field_ref[part, pl.ds(at, rows), :]
    cos_part, sin_part = analysed_right(jnp.concatenate(start, axis=0), Table(table_ref))
    real, imag = cos_part[:held] + sin_part[held:], cos_part[held:] - sin_part[:held]
    for tile in range(real.shape[1] // LANES):
        lanes = slice(tile * LANES, (tile + 1) * LANES)
        for at, block in enumerate(swap_halves(real[:, lanes], imag[:, lanes])):
            out_ref[pl.ds((2 * tile + at) * held, held), :] = block


def assemble_kernel(*refs, rows):
    pieces, (parts_ref, tail_ref, head_ref) = refs[:GROUPS], refs[GROUPS:]
    group = my_group()[0]
    for shift in range(GROUPS):
        source = lax.rem(group - shift + GROUPS, GROUPS)
        for part in range(2):
            value = pieces[shift][part]
            parts_ref[part * GROUPS + source] = value
            tail_ref[part * GROUPS + source] = value[rows - HALF :]
            head_ref[part * GROUPS + source] = value[:HALF]


def end_kernel(in_ref, lens_ref, params_ref, table_ref, flip_ref, *out_refs, rows):
    parts_ref, tail_ref, head_ref = out_refs
    first, second = inverse_rows(in_ref, Table(table_ref, flip_ref), GROUPS, rows)
    weight = params_ref[pl.ds(rows, rows), :]
    for group in range(GROUPS):
        lens_sin = lens_ref[1, group % 2]
        field = lensed(
            first[group],
            second[group],
            weight,
            lens_ref[0, group % 2],
            lens_sin if group >= 2 else -lens_sin,
        )
        for part in range(2):
            parts_ref[part * GROUPS + group] = field[part]
            tail_ref[part * GROUPS + group] = field[part][rows - HALF :]
            head_ref[part * GROUPS + group] = field[part][:HALF]


def image_body(field_ref, above_ref, below_ref, base_ref, out_ref, padded_ref, rows):
    for index in range(8):
        padded_ref[index, pl.ds(0, HALF)] = above_ref[index]
        padded_ref[index, pl.ds(HALF, rows)] = field_ref[index]
        padded_ref[index, pl.ds(HALF + rows, HALF)] = below_ref[index]
    for lag in range(LAGS):
        offset = lag - HALF
        total = None if base_ref is None else base_ref[lag]
        for part in range(2):
            for freq in range(2):
                source = padded_ref[part * 4 + freq, pl.ds(HALF - offset, rows)]
                receiver = padded_ref[part * 4 + 2 + freq, pl.ds(HALF + offset, rows)]
                total = source * receiver if total is None else total + source * receiver
        out_ref[lag] = total


def image_first(field_ref, above_ref, below_ref, out_ref, padded_ref, *, rows):
    image_body(field_ref, above_ref, below_ref, None, out_ref, padded_ref, rows)


def image_second(field_ref, above_ref, below_ref, base_ref, out_ref, padded_ref, *, rows):
    image_body(field_ref, above_ref, below_ref, base_ref, out_ref, padded_ref, rows)


def store_kernel(in_ref, out_ref):
    out_ref[...] = in_ref[...]


VMEM = pl.BlockSpec(memory_space=pltpu.VMEM)
SMEM = pl.BlockSpec(memory_space=pltpu.SMEM)


def call(kernel, in_specs, out_shapes, operands, flops, scratch=(), **params):
    many = len(out_shapes) > 1
    shapes = [jax.ShapeDtypeStruct(shape, jnp.float32) for shape in out_shapes]
    return pl.pallas_call(
        functools.partial(kernel, **params),
        in_specs=in_specs,
        out_specs=[VMEM] * len(shapes) if many else VMEM,
        out_shape=shapes if many else shapes[0],
        scratch_shapes=list(scratch),
        cost_estimate=pl.CostEstimate(flops=flops, bytes_accessed=1 << 20, transcendentals=0),
        compiler_params=pltpu.CompilerParams(vmem_limit_bytes=24 << 20),
        interpret=INTERPRET,
    )(*operands)


def shards(
    fields, surface, held_freqs, surface_freqs, ref_slowness, weights, regions, region_slowness
):
    lane_count = lax.axis_size("lat")
    sections = lax.axis_size("depth")
    rows, col_length = fields.shape[4], fields.shape[5]
    length = lane_count * rows
    members = lane_count // GROUPS
    held = GROUPS * rows
    tables_y = transform_tables(col_length)
    tables_x = tables_y if length == col_length else transform_tables(length)
    groups = [[group * members + i for i in range(members)] for group in range(GROUPS)]
    held_freqs = held_freqs[0]

    def exchanged(value, within=None):
        return lax.all_to_all(
            value, "lat", split_axis=0, concat_axis=0, tiled=True, axis_index_groups=within
        )

    def across(pieces):
        moved = [pieces[0]]
        for shift in range(1, GROUPS):
            pairs = [(i, (i + shift * members) % lane_count) for i in range(lane_count)]
            moved.append(lax.ppermute(pieces[shift], "lat", pairs))
        return moved

    def factors(params, tick):
        shape = (length, LANES)
        return call(
            factor_kernel,
            [SMEM, SMEM, VMEM],
            [shape, shape],
            (held_freqs, surface_freqs, params),
            1 << 27,
            tick=tick,
            length=length,
            rows=rows,
        )

    def columns(value, pair, tick):
        return call(
            columns_kernel,
            [VMEM] * 5,
            [(length, 2 * LANES)],
            (value, *pair, *tables_x),
            1 << 29,
            rows=rows,
            tick=tick,
        )

    padded = [pltpu.VMEM((8, rows + 2 * HALF, col_length), jnp.float32)]
    image_shape = (LAGS, rows, col_length)
    parts_shape, edge_shape = (8, rows, col_length), (8, HALF, col_length)
    packed_shape, params_shape = (4 * rows, col_length), (2 * rows + 16, col_length)

    spectra = call(
        rows_kernel,
        [VMEM] * 2,
        [(length, LANES)],
        (fields.reshape(8 * rows, col_length), tables_y[0]),
        1 << 28,
        rows=rows,
    )
    *packed, params = call(
        prepare_kernel,
        [VMEM, SMEM, VMEM, SMEM, VMEM],
        [packed_shape] * GROUPS + [params_shape],
        (
            regions[0, 0],
            region_slowness[0, 0],
            weights[0, 0],
            ref_slowness[0, 0],
            surface.reshape(parts_shape),
        ),
        1 << 24,
        rows=rows,
    )
    entered = exchanged(spectra)
    packed = across(packed)
    pair = factors(params, 0)
    shifted = columns(entered, pair, 0)
    returned = exchanged(shifted, groups)
    upward = [(s, (s - 1) % sections) for s in range(sections)]
    passed = lax.ppermute(params, "depth", upward)
    weight, lenses, start = call(
        gather_kernel,
        [SMEM] + [VMEM] * GROUPS,
        [(held, col_length), (2, held, col_length), (2, held, col_length)],
        (held_freqs, *packed),
        1 << 25,
        rows=rows,
    )
    next_pair = factors(passed, 1)
    spectra, *pieces = call(
        turn_kernel,
        [VMEM] * 6,
        [(length, LANES)] + [(2, rows, col_length)] * GROUPS,
        (returned, weight, lenses, start, *tables_y),
        1 << 29,
        [pltpu.VMEM((2, held, col_length), jnp.float32)],
        rows=rows,
    )
    spectra = exchanged(spectra, groups)
    pieces = across(pieces)

    def along(step):
        return [(i, i + step) for i in range(lane_count) if 0 <= i + step < lane_count]

    parts, tail, head = call(
        assemble_kernel,
        [VMEM] * GROUPS,
        [parts_shape, edge_shape, edge_shape],
        pieces,
        1 << 20,
        rows=rows,
    )
    above = lax.ppermute(tail, "lat", along(1))
    below = lax.ppermute(head, "lat", along(-1))
    image = call(
        image_first, [VMEM] * 3, [image_shape], (parts, above, below), 1 << 26, padded, rows=rows
    )
    shifted = columns(spectra, next_pair, 1)
    returned = exchanged(shifted)
    lenses = call(
        lens_kernel,
        [SMEM, SMEM, VMEM],
        [(2, 2, rows, col_length)],
        (held_freqs, surface_freqs, passed),
        1 << 24,
        rows=rows,
    )
    parts, tail, head = call(
        end_kernel,
        [VMEM] * 5,
        [parts_shape, edge_shape, edge_shape],
        (returned, lenses, passed, *tables_y),
        1 << 29,
        rows=rows,
    )

    def diagonal(step):
        return [
            (s * lane_count + i, (s + 1) % sections * lane_count + i + step)
            for s in range(sections)
            for i in range(lane_count)
            if 0 <= i + step < lane_count
        ]

    above = lax.ppermute(tail, ("depth", "lat"), diagonal(1))
    below = lax.ppermute(head, ("depth", "lat"), diagonal(-1))
    parts = lax.ppermute(parts, ("depth", "lat"), diagonal(0))
    image = call(
        image_second,
        [VMEM] * 4,
        [image_shape],
        (parts, above, below, image),
        1 << 26,
        padded,
        rows=rows,
    )
    stored = call(store_kernel, [VMEM], [parts_shape], (parts,), 1 << 20)
    return (stored.reshape(fields.shape), image[None, None])


def solution(mesh):
    in_specs = (
        P("depth", None, None, None, "lat", None),
        P(None, None, None, "lat", None),
        P("depth", None),
        P(),
        P("depth", None, None),
        P("depth", None, "lat", None),
        P("depth", None, "lat", None),
        P("depth", None, None),
    )
    out_specs = (P("depth", None, None, None, "lat", None), P("depth", None, None, "lat", None))


    return jax.shard_map(shards, mesh=mesh, in_specs=in_specs, out_specs=out_specs, check_vma=False)
```
